32 devices in a mesh: dp: 4 (over z), rows: 8 (over y, x, core).
Axes of the slice: x: 2, y: 2, z: 4, core: 2. Of those that a mesh axis runs over, the one named last changes fastest.
Arguments:
- latent: bfloat16 [8, 8, 64, 640], P('dp', 'rows'), may hold values from -16.25 to 16.25
- hidden: bfloat16 [8, 8, 64, 640], P('dp', 'rows'), may hold values from -16.25 to 16.25
- cotangent: bfloat16 [8, 8, 64, 640], P('dp', 'rows'), may hold values from -6 to 6
- filter_one: bfloat16 [9, 640, 640], P(None, 'dp', 'rows'), may hold values from -0.078125 to 0.078125
- filter_two: bfloat16 [9, 640, 640], P(None, 'dp', 'rows'), may hold values from -0.078125 to 0.078125
- gain_one: float32 [640], replicated, may hold values from 0.1 to 1.9
- shift_one: float32 [640], replicated, may hold values from -2.5 to 2.5
- gain_two: float32 [640], replicated, may hold values from 0.1 to 1.9
- shift_two: float32 [640], replicated, may hold values from -2.5 to 2.5
Outputs:
- latent_grad: bfloat16 [8, 8, 64, 640], P('dp', 'rows')
The draws below stay inside these ranges and needn't reach their ends.
All inputs are finite; a program needn't handle non-finite values.
Results may differ from the reference program's by a relative error of at most 0.0027.
Values may be sent and summed in bfloat16 or wider, within the bound.
No kernel may reach another device: no remote copies, remote signals or barrier semaphores. Data moves between devices by JAX's collectives and lax.ppermute only.
A program may use at most 128 MiB of HBM per device.

```python
import jax
import jax.numpy as jnp
from jax import lax

GROUPS = 16
GSIZE = 40
WIDTH = 64
CH = 640
IMAGES = 8
HEIGHT = 8


def draw_field(key, salt):
    key = jax.random.fold_in(key, salt)
    key_noise, key_channel = jax.random.split(key, 2)
    height_pos = jnp.arange(HEIGHT, dtype=jnp.float32) / max(HEIGHT - 1, 1)
    row_scale = jnp.exp(jnp.log(3.0) * height_pos)[None, :, None, None]
    channel_scale = jnp.exp(jax.random.uniform(key_channel, (CH,), jnp.float32, jnp.log(0.1), 0.0))
    noise = jnp.clip(jax.random.normal(key_noise, (IMAGES, HEIGHT, WIDTH, CH), jnp.float32), -5.0, 5.0)
    field = noise * row_scale * channel_scale
    return field.astype(jnp.bfloat16)


def draw_latent(key, part):
    return draw_field(key, 11)


def draw_hidden(key, part):
    return draw_field(key, 23)


def draw_cotangent(key, part):
    key = jax.random.fold_in(key, 37)
    key_noise, key_offset = jax.random.split(key, 2)
    noise = jax.random.normal(key_noise, (IMAGES, HEIGHT, WIDTH, CH), jnp.float32)
    offset = jax.random.normal(key_offset, (IMAGES, 1, 1, CH), jnp.float32)
    field = jnp.clip(noise + offset, -6.0, 6.0)
    return field.astype(jnp.bfloat16)


def levels(key, dims, cuts, low, top_value):
    factor_of, own = 1.0, jax.random.fold_in(key, 6)
    for axis_at, blocks in cuts:
        draws = jnp.exp(jax.random.uniform(jax.random.fold_in(own, axis_at), (blocks,), jnp.float32, low / len(cuts), top_value / len(cuts)))
        factor_of = factor_of * jnp.repeat(draws, dims[axis_at] // blocks).reshape([-1 if axis == axis_at else 1 for axis in range(len(dims))])
    return factor_of


def centred(stream_key, extent, scale, most, cuts=(), held_as=jnp.bfloat16):
    level = levels(stream_key, extent, cuts, -0.22, 0.18) if cuts else 1.0
    values = jax.random.normal(stream_key, extent, jnp.float32) * scale * level
    return jnp.minimum(jnp.maximum(values, -most), most).astype(held_as)


def setup_inputs(seed: int = 0) -> dict:
    seeds = jax.random.split(jax.random.key(seed), 10)
    return {
        "latent": draw_latent(jax.random.fold_in(seeds[9], 71), 0),
        "hidden": draw_hidden(jax.random.fold_in(seeds[9], 71), 0),
        "cotangent": draw_cotangent(jax.random.fold_in(seeds[9], 71), 0),
        "filter_one": centred(seeds[3], (9, CH, CH), (9 * CH) ** -0.5, 0.078125, ((1, 4), (2, 8))),
        "filter_two": centred(seeds[4], (9, CH, CH), (9 * CH) ** -0.5, 0.078125, ((1, 4), (2, 8))),
        "gain_one": jnp.clip(1.0 + 0.18 * jax.random.normal(seeds[5], (CH,), jnp.float32), 0.1, 1.9),
        "shift_one": centred(seeds[6], (CH,), 0.5, 2.5, (), jnp.float32),
        "gain_two": jnp.clip(1.0 + 0.18 * jax.random.normal(seeds[7], (CH,), jnp.float32), 0.1, 1.9),
        "shift_two": centred(seeds[8], (CH,), 0.5, 2.5, (), jnp.float32),
    }


def group_sums(values):
    per_channel = lax.optimization_barrier(jnp.sum(values, axis=(1, 2)))
    return lax.optimization_barrier(jnp.sum(per_channel.reshape(per_channel.shape[0], GROUPS, -1), axis=2))

def expand_groups(moment):
    return jnp.repeat(moment, GSIZE, axis=1)[:, None, None, :]

def finish_stats(sum_plain, sum_square, number):
    average = sum_plain / number
    variance = sum_square / number - average * average
    return (average, lax.rsqrt(variance + 1e-05))

def norm_backward(field, stats, gain, shift, incoming, number):
    average, inverse = stats
    values = field.astype(jnp.float32)
    normed = (values - expand_groups(average)) * expand_groups(inverse)
    linear = normed * gain + shift
    logistic = jax.nn.sigmoid(linear)
    scaled = incoming * logistic * (1.0 + linear * (1.0 - logistic)) * gain
    first = group_sums(scaled) / number
    second = group_sums(scaled * normed) / number
    return expand_groups(inverse) * (scaled - expand_groups(first) - normed * expand_groups(second))

def conv_backward(gradient, weights):
    images, height, breadth, channels = gradient.shape
    padded = jnp.pad(gradient, ((0, 0), (1, 1), (1, 1), (0, 0)))
    result = jnp.zeros((images * height * breadth, channels), jnp.float32)
    for tap_index in range(9):
        down_step = tap_index // 3 - 1
        side_step = tap_index % 3 - 1
        window = padded[:, 1 - down_step:1 - down_step + height, 1 - side_step:1 - side_step + breadth, :]
        window = window.reshape(images * height * breadth, channels)
        result = result + jnp.dot(window, weights[tap_index].T, preferred_element_type=jnp.float32)
    return result.reshape(images, height, breadth, channels)

def reference(latent, hidden, cotangent, filter_one, filter_two, gain_one, shift_one, gain_two, shift_two):
    number = HEIGHT * WIDTH * GSIZE
    latent_values = latent.astype(jnp.float32)
    hidden_values = hidden.astype(jnp.float32)
    stats_one = finish_stats(group_sums(latent_values), group_sums(latent_values * latent_values), number)
    stats_two = finish_stats(group_sums(hidden_values), group_sums(hidden_values * hidden_values), number)
    back_two = conv_backward(cotangent, filter_two)
    hidden_grad = norm_backward(hidden, stats_two, gain_two, shift_two, back_two, number).astype(jnp.bfloat16)
    back_one = conv_backward(hidden_grad, filter_one)
    latent_part = norm_backward(latent, stats_one, gain_one, shift_one, back_one, number)
    return (cotangent.astype(jnp.float32) + latent_part).astype(jnp.bfloat16)
```

```python
import functools

import jax
import jax.numpy as jnp
from jax import lax
from jax.experimental import pallas as pl
from jax.experimental.pallas import tpu as pltpu
from jax.sharding import PartitionSpec as P

GROUPS = 16
GSIZE = 40
LANES = 128


F32 = jnp.float32
BF16 = jnp.bfloat16


def up(number, unit):
    return -(-number // unit) * unit


def full_specs(count, space):
    return [pl.BlockSpec(memory_space=space) for _ in range(count)]


def one_hot(source, target):
    return jnp.where(source == target, 1.0, 0.0).astype(BF16)


def dot(left, right):
    return jnp.dot(left, right, preferred_element_type=F32)


def iota(shape, axis):
    return lax.broadcasted_iota(jnp.int32, shape, axis)


def pack_filter_kernel(place, taps, *outs, blocks):
    chunk = taps.shape[2]
    position = place[1]
    parts = []
    for block in range(blocks):
        rows = []
        for down in range(3):
            pieces = [
                taps[3 * down + side, block * GSIZE : (block + 1) * GSIZE, :].astype(F32)
                for side in range(3)
            ]
            pieces.append(jnp.zeros((LANES - 3 * GSIZE, chunk), F32))
            rows.append(jnp.concatenate(pieces, axis=0).T.astype(BF16))
        parts.append(rows)
    for step, out in enumerate(outs):
        wanted = position ^ step
        for down in range(3):
            value = parts[0][down]
            for block in range(1, blocks):
                value = jnp.where(wanted == block, parts[block][down], value)
            out[down] = value


def pack_filter(place, taps, blocks):
    chunk = taps.shape[2]
    return pl.pallas_call(
        functools.partial(pack_filter_kernel, blocks=blocks),
        out_shape=[jax.ShapeDtypeStruct((3, chunk, LANES), BF16)] * blocks,
        in_specs=[
            pl.BlockSpec(memory_space=pltpu.SMEM),
            pl.BlockSpec(memory_space=pltpu.VMEM),
        ],
        out_specs=full_specs(blocks, pltpu.VMEM),
        name="pack_filter",
    )(place, taps)


def channel_of(order, inner, strides, position, outer):
    return (order ^ outer) * strides[0] + position * strides[1] + inner


def pack_fields_kernel(place, cotangent, hidden, latent, out, *, blocks, per_block, strides, twist):
    images, width, channels = cotangent.shape
    field_lanes = out.shape[2] - channels
    outer = place[0] * twist
    rows = iota((channels, field_lanes), 0)
    lane = iota((channels, field_lanes), 1)
    own = per_block * GSIZE
    for block in range(blocks):
        mixed = jnp.zeros((images * width, field_lanes), F32)
        for at, field in enumerate((hidden, latent)):
            local = lane - at * own
            order = local // GSIZE
            channel = channel_of(order, local - order * GSIZE, strides, block, outer)
            inside = (local >= 0) & (local < own)
            select = one_hot(rows, jnp.where(inside, channel, -1))
            mixed = mixed + dot(field[...].reshape(images * width, channels), select)
        mixed = mixed.astype(BF16).reshape(images, width, field_lanes)
        for image in range(images):
            out[block * images + image, :, :channels] = cotangent[image]
            out[block * images + image, :, channels:] = mixed[image]


def group_total(values):
    return jnp.sum(jnp.sum(values, axis=0, keepdims=True), axis=1, keepdims=True)


def convolve(weights, padded, width):
    rows = padded.shape[0] - 2 * width
    total = None
    for down in range(3):
        window = padded[(2 - down) * width : (2 - down) * width + rows, :]
        term = dot(window, weights[down])
        total = term if total is None else total + term
    return total


def fold_sides(total, width):
    rows = total.shape[0]
    column = lax.rem(iota((rows, LANES), 0), width)
    first = jnp.where(column == width - 1, 0.0, pltpu.roll(total, rows - 1, 0))
    last = pltpu.roll(pltpu.roll(total, LANES - 2 * GSIZE, 1), 1, 0)
    last = jnp.where(column == 0, 0.0, last)
    return first + pltpu.roll(total, LANES - GSIZE, 1) + last


def norm_backward(values, incoming, gain, shift, number):
    average = group_total(values) / number
    inverse = lax.rsqrt(group_total(values * values) / number - average * average + 1e-05)
    normed = (values - average) * inverse
    linear = normed * gain + shift
    logistic = 1.0 / (1.0 + jnp.exp(-linear))
    scaled = incoming * logistic * (1.0 + linear * (1.0 - logistic)) * gain
    first = group_total(scaled) / number
    second = group_total(scaled * normed) / number
    return inverse * (scaled - first - normed * second)


def load_weights(place, pieces, weights, semaphore):
    copies = []
    position, core = place[1], place[2]
    cores = len(pieces)
    for swap, by_order in enumerate(pieces):
        for order, arrays in enumerate(by_order):
            step = 0
            for array in arrays:
                for inner in range(array.shape[0]):
                    chunk = array.shape[2]
                    source = (position ^ step) * cores + (core ^ swap)
                    start = pl.multiple_of(source * chunk, 16)
                    copies.append(
                        pltpu.make_async_copy(
                            array.at[inner],
                            weights.at[:, pl.ds(start, chunk), pl.ds(order * LANES, LANES)],
                            semaphore,
                        )
                    )
                    step += 1
    for copy in copies:
        copy.start()
    return copies


def field_select(field_lanes, per_block, at):
    rows = iota((field_lanes, per_block * LANES), 0)
    lane = iota((field_lanes, per_block * LANES), 1)
    inner = lane % LANES
    return one_hot(rows, jnp.where(inner < GSIZE, (at * per_block + lane // LANES) * GSIZE + inner, -1))


def fold_select(lanes, order, half, per_block):
    rows = iota((LANES, lanes), 0)
    lane = iota((LANES, lanes), 1)
    local = lane - (half * per_block + order) * GSIZE
    return one_hot(rows, jnp.where((local >= 0) & (local < GSIZE), local, -1))


def hidden_kernel(place, received, gain, shift, *rest, layout, number, per_block):
    flat = rest[: layout.total]
    out, padded, weights, semaphore = rest[layout.total :]
    copies = load_weights(place, layout.nest(flat), weights, semaphore) if layout.dynamic else []
    height, width, lanes = received.shape
    channels = padded.shape[1]
    rows = height * width
    fields = received[:, :, channels:].reshape(rows, lanes - channels)
    padded[:width, :] = jnp.zeros((width, channels), BF16)
    padded[width + rows :, :] = jnp.zeros((width, channels), BF16)
    padded[width : width + rows, :] = received[:, :, :channels].reshape(rows, channels)
    values = dot(fields, field_select(lanes - channels, per_block, 0))
    for copy in copies:
        copy.wait()
    total = convolve(weights if layout.dynamic else flat[0], padded, width)
    half_rows = rows // 2
    packed = jnp.zeros((half_rows, out.shape[1]), F32)
    for order in range(per_block):
        part = slice(order * LANES, (order + 1) * LANES)
        incoming = fold_sides(total[:, part], width)
        grad = norm_backward(values[:, part], incoming, gain[:, part], shift[:, part], number)
        grad = grad.astype(BF16)
        for half in range(2):
            piece = grad[half * half_rows : (half + 1) * half_rows]
            packed = packed + dot(piece, fold_select(out.shape[1], order, half, per_block))
    out[...] = packed.astype(BF16)


def latent_kernel(place, received, gain, shift, *rest, layout, number, per_block, blocks, strides, twist):
    grads = rest[:blocks]
    flat = rest[blocks : blocks + layout.total]
    out, padded, weights, semaphore = rest[blocks + layout.total :]
    copies = load_weights(place, layout.nest(flat), weights, semaphore) if layout.dynamic else []
    height, width, lanes = received.shape
    channels = padded.shape[1]
    rows = height * width
    half_rows = rows // 2
    outer, position = place[0] * twist, place[1]
    padded[:width, :] = jnp.zeros((width, channels), BF16)
    padded[width + rows :, :] = jnp.zeros((width, channels), BF16)
    folded = grads[0].shape[1]
    row = iota((folded, channels), 0)
    column = iota((folded, channels), 1)
    own = per_block * GSIZE
    for half in range(2):
        total = jnp.zeros((half_rows, channels), F32)
        for step, grad in enumerate(grads):
            local = row - half * own
            order = local // GSIZE
            channel = channel_of(order, local - order * GSIZE, strides, position ^ step, outer)
            inside = (local >= 0) & (local < own)
            total = total + dot(grad[...], one_hot(jnp.where(inside, channel, -1), column))
        padded[width + half * half_rows : width + (half + 1) * half_rows, :] = total.astype(BF16)
    fields = received[:, :, channels:].reshape(rows, lanes - channels)
    values = dot(fields, field_select(lanes - channels, per_block, 1))
    row = iota((channels, per_block * LANES), 0)
    lane = iota((channels, per_block * LANES), 1)
    inner = lane % LANES
    channel = channel_of(lane // LANES, inner, strides, position, outer)
    straight = received[:, :, :channels].reshape(rows, channels)
    straight = dot(straight, one_hot(row, jnp.where(inner < GSIZE, channel, -1)))
    for copy in copies:
        copy.wait()
    total = convolve(weights if layout.dynamic else flat[0], padded, width)
    half_width = width // 2
    packed = jnp.zeros((height * half_width, out.shape[2]), F32)
    for order in range(per_block):
        part = slice(order * LANES, (order + 1) * LANES)
        incoming = fold_sides(total[:, part], width)
        grad = norm_backward(values[:, part], incoming, gain[:, part], shift[:, part], number)
        grad = (straight[:, part] + grad).astype(BF16).reshape(height, width, LANES)
        for half in range(2):
            piece = grad[:, half * half_width : (half + 1) * half_width, :]
            piece = piece.reshape(height * half_width, LANES)
            packed = packed + dot(piece, fold_select(out.shape[2], order, half, per_block))
    out[...] = packed.astype(BF16).reshape(height, half_width, out.shape[2])


def spread_kernel(place, received, out, *, images, per_block, strides, twist):
    sources, half_width, folded = received.shape
    channels = out.shape[2]
    outer = place[0] * twist
    row = iota((folded, channels), 0)
    column = iota((folded, channels), 1)
    own = per_block * GSIZE
    blocks = sources // images
    for half in range(2):
        totals = [jnp.zeros((half_width, channels), F32) for _ in range(images)]
        for block in range(blocks):
            local = row - half * own
            order = local // GSIZE
            channel = channel_of(order, local - order * GSIZE, strides, block, outer)
            inside = (local >= 0) & (local < own)
            select = one_hot(jnp.where(inside, channel, -1), column)
            for image in range(images):
                totals[image] = totals[image] + dot(received[block * images + image], select)
        for image in range(images):
            out[image, half * half_width : (half + 1) * half_width, :] = totals[image].astype(BF16)


class Layout:
    def __init__(self, pieces):
        self.dynamic = isinstance(pieces, list)
        if self.dynamic:
            self.counts = [[len(arrays) for arrays in by_order] for by_order in pieces]
            self.flat = [array for by_order in pieces for arrays in by_order for array in arrays]
        else:
            self.flat = [pieces]
        self.total = len(self.flat)

    def nest(self, flat):
        flat, result = list(flat), []
        for counts in self.counts:
            result.append([[flat.pop(0) for _ in range(count)] for count in counts])
        return result


def flip(array, axis, mask):
    return lax.ppermute(array, axis, [(i, i ^ mask) for i in range(lax.axis_size(axis))])


def gathered_filter(place, taps, blocks, images):
    mine = pack_filter(place, taps, blocks)
    mine = [mine[0]] + [flip(mine[step], "rows", step * images) for step in range(1, blocks)]
    halves = [jnp.stack(mine[: blocks // 2]), jnp.stack(mine[blocks // 2 :])]
    far = [flip(half, "dp", 2) for half in halves]
    near = [flip(half, "dp", 1) for half in halves]
    last = [flip(half, "dp", 1) for half in far]
    own = [halves, near, far, last]
    swapped = [[flip(half, "rows", 1) for half in pair] for pair in own]
    return [own, swapped]


def assembled_filter(place, taps, blocks, per_block, images):
    count, _, chunk = taps.shape
    whole = lax.all_gather(taps, "dp", axis=1, tiled=True)
    sources = lax.axis_size("rows")
    whole = whole.reshape(count, blocks, per_block * GSIZE, chunk)
    whole = jnp.repeat(jnp.moveaxis(whole, 1, 0), images, axis=0)
    whole = lax.all_to_all(whole, "rows", 0, 0, tiled=True)
    whole = whole.reshape(sources, 3, 3, per_block, GSIZE, chunk)
    whole = jnp.transpose(whole, (1, 0, 5, 3, 2, 4)).reshape(3, sources * chunk, per_block, 3 * GSIZE)
    whole = jnp.pad(whole, ((0, 0), (0, 0), (0, 0), (0, LANES - 3 * GSIZE)))
    return whole.reshape(3, sources * chunk, per_block * LANES)


def body(
    latent, hidden, cotangent, filter_one, filter_two, gain_one, shift_one, gain_two, shift_two
):
    images, _, width, channels = latent.shape
    height, planes = lax.axis_size("rows"), lax.axis_size("dp")
    blocks = height // images
    per_block = GROUPS // blocks
    fast = planes == 4 and images == 2 and blocks == 4 and per_block == planes
    twist = 1 if fast else 0
    strides = (channels // planes, GSIZE) if fast else (GSIZE, per_block * GSIZE)
    number = float(height * width * GSIZE)
    rows = height * width
    plane, here = lax.axis_index("dp"), lax.axis_index("rows")
    position, core = here // images, here % images
    place = jnp.stack([plane, position, core]).astype(jnp.int32)
    smem = pl.BlockSpec(memory_space=pltpu.SMEM)
    vmem = pl.BlockSpec(memory_space=pltpu.VMEM)

    def filter_pieces(taps):
        if fast:
            return gathered_filter(place, taps, blocks, images)
        return assembled_filter(place, taps, blocks, per_block, images)

    def per_lane(vector):
        if fast:
            grouped = vector.reshape(planes, blocks, GSIZE)
            grouped = jnp.take(grouped, position, axis=1)
            grouped = jnp.take(grouped, jnp.arange(planes) ^ plane, axis=0)
        else:
            grouped = jnp.take(vector.reshape(blocks, per_block, GSIZE), position, axis=0)
        grouped = jnp.pad(grouped, ((0, 0), (0, LANES - GSIZE)))
        return grouped.reshape(1, per_block * LANES)

    field_lanes = up(2 * per_block * GSIZE, LANES)
    pieces_two = Layout(filter_pieces(filter_two))
    sent = pl.pallas_call(
        functools.partial(
            pack_fields_kernel,
            blocks=blocks,
            per_block=per_block,
            strides=strides,
            twist=twist,
        ),
        out_shape=jax.ShapeDtypeStruct((height, width, channels + field_lanes), BF16),
        in_specs=[smem, vmem, vmem, vmem],
        out_specs=vmem,
        name="pack_fields",
    )(place, cotangent[:, 0], hidden[:, 0], latent[:, 0])
    received = lax.all_to_all(sent, "rows", 0, 0, tiled=True)
    pieces_one = Layout(filter_pieces(filter_one))

    def scratch(layout):
        return [
            pltpu.VMEM(((height + 2) * width, channels), BF16),
            pltpu.VMEM((3, channels, per_block * LANES), BF16) if layout.dynamic else pltpu.VMEM((8, LANES), F32),
            pltpu.SemaphoreType.DMA(()),
        ]

    folded = up(2 * per_block * GSIZE, LANES)

    def specs(layout):
        return full_specs(layout.total, pl.ANY if layout.dynamic else pltpu.VMEM)

    grad = pl.pallas_call(
        functools.partial(hidden_kernel, layout=pieces_two, number=number, per_block=per_block),
        out_shape=jax.ShapeDtypeStruct((rows // 2, folded), BF16),
        in_specs=[smem, vmem, vmem, vmem] + specs(pieces_two),
        out_specs=vmem,
        scratch_shapes=scratch(pieces_two),
        name="hidden_side",
    )(place, received, per_lane(gain_two), per_lane(shift_two), *pieces_two.flat)
    grads = [grad] + [flip(grad, "rows", step * images) for step in range(1, blocks)]
    result = pl.pallas_call(
        functools.partial(
            latent_kernel,
            layout=pieces_one,
            number=number,
            per_block=per_block,
            blocks=blocks,
            strides=strides,
            twist=twist,
        ),
        out_shape=jax.ShapeDtypeStruct((height, width // 2, folded), BF16),
        in_specs=[smem, vmem, vmem, vmem] + [vmem] * blocks + specs(pieces_one),
        out_specs=vmem,
        scratch_shapes=scratch(pieces_one),
        name="latent_side",
    )(place, received, per_lane(gain_one), per_lane(shift_one), *grads, *pieces_one.flat)
    result = lax.all_to_all(result, "rows", 0, 0, tiled=True)
    out = pl.pallas_call(
        functools.partial(
            spread_kernel, images=images, per_block=per_block, strides=strides, twist=twist
        ),
        out_shape=jax.ShapeDtypeStruct((images, width, channels), BF16),
        in_specs=[smem, vmem],
        out_specs=vmem,
        name="spread",
    )(place, result)
    return out[:, None]


def solution(mesh):
    in_specs = (
        P("dp", "rows", None, None),
        P("dp", "rows", None, None),
        P("dp", "rows", None, None),
        P(None, "dp", "rows"),
        P(None, "dp", "rows"),
        P(),
        P(),
        P(),
        P(),
    )
    out_specs = P("dp", "rows", None, None)
    return jax.shard_map(body, mesh=mesh, in_specs=in_specs, out_specs=out_specs, check_vma=False)
```

```python
import functools

import jax
import jax.numpy as jnp
from jax import lax
from jax.experimental import pallas as pl
from jax.experimental.pallas import tpu as pltpu
from jax.sharding import PartitionSpec as P


GROUPS = 16
GSIZE = 40
LANES = 128


CHUNKS_TWO = ((0,), (1,), (2, 3))
CHUNKS_ONE = ((0, 1), (2, 3))

F32 = jnp.float32
BF16 = jnp.bfloat16


def up(number, unit):
    return -(-number // unit) * unit


def one_hot(source, target):
    return jnp.where(source == target, 1.0, 0.0).astype(BF16)


def dot(left, right):
    return jnp.dot(left, right, preferred_element_type=F32)


def iota(shape, axis):
    return lax.broadcasted_iota(jnp.int32, shape, axis)


class Plan:
    def __init__(self, images, width, channels):
        self.images, self.width, self.channels = images, width, channels
        self.height, self.planes = lax.axis_size("rows"), lax.axis_size("dp")
        self.rows = self.height * width
        self.blocks = self.height // images
        self.per_block = GROUPS // self.blocks
        self.number = float(self.rows * GSIZE)
        self.fast = (
            self.planes == 4 and images == 2 and self.blocks == 4 and self.per_block == self.planes
        )
        self.lanes = self.per_block * LANES
        self.field_lanes = up(2 * self.per_block * GSIZE, LANES)
        three = LANES // GSIZE
        self.mains = [
            list(range(start, min(start + three, self.per_block)))
            for start in range(0, self.per_block, three)
        ]
        self.spare = self.mains.pop()[0] if len(self.mains[-1]) == 1 else None

    def packed_rows(self, rows):
        return len(self.mains) * rows + (rows // 2 if self.spare is not None else 0)

    def place(self):
        here = lax.axis_index("rows")
        return lax.axis_index("dp"), here // self.images, here % self.images

    def channel(self, plane, block, order):
        if self.fast:
            return (order ^ plane) * (self.channels // self.planes) + block * GSIZE
        return (block * self.per_block + order) * GSIZE

    def targets(self, index, spans):
        target = jnp.full(index.shape, -1, jnp.int32)
        for start, channel in spans:
            inside = (index >= start) & (index < start + GSIZE)
            target = jnp.where(inside, channel + index - start, target)
        return target


def call(body, out, inputs, held=(), scratch=(), space=pltpu.VMEM):
    kinds = {pltpu.VMEM: pltpu.VMEM, pl.ANY: jax.ShapeDtypeStruct}
    outs = [kinds[space](shape, dtype) for shape, dtype in out]
    inputs = [
        pltpu.with_memory_space_constraint(value, pltpu.VMEM) if at in held else value
        for at, value in enumerate(inputs)
    ]
    vmem = pl.BlockSpec(memory_space=pltpu.VMEM)
    return pl.pallas_call(
        body,
        out_shape=outs,
        in_specs=[vmem] * len(inputs),
        out_specs=[vmem] * len(outs),
        scratch_shapes=list(scratch),
        compiler_params=pltpu.CompilerParams(vmem_limit_bytes=24 * 1024 * 1024),
    )(*inputs)


def pack_filters_kernel(first, second, *outs, plan):
    chunk = first.shape[2]
    position = plan.place()[1]
    for at, taps in enumerate((first, second)):
        parts = []
        for block in range(plan.blocks):
            rows = []
            for down in range(3):
                pieces = [
                    taps[3 * down + side, block * GSIZE : (block + 1) * GSIZE, :].astype(F32)
                    for side in range(3)
                ]
                pieces.append(jnp.zeros((LANES - 3 * GSIZE, chunk), F32))
                rows.append(jnp.concatenate(pieces, axis=0).T.astype(BF16))
            parts.append(rows)
        for step, out in enumerate(outs):
            wanted = position ^ step
            for down in range(3):
                value = parts[0][down]
                for block in range(1, plan.blocks):
                    value = jnp.where(wanted == block, parts[block][down], value)
                out[at, down] = value


def pack_fields_kernel(cotangent, hidden, latent, out, *, plan):
    plane = plan.place()[0]
    images, width, channels = cotangent.shape
    rows = iota((channels, 1), 0)
    lane = iota((1, plan.field_lanes), 1)
    own = plan.per_block * GSIZE
    for block in range(plan.blocks):
        mixed = jnp.zeros((images * width, plan.field_lanes), F32)
        for at, field in enumerate((hidden, latent)):
            spans = [
                (at * own + order * GSIZE, plan.channel(plane, block, order))
                for order in range(plan.per_block)
            ]
            select = one_hot(rows, plan.targets(lane, spans))
            mixed = mixed + dot(field[...].reshape(images * width, channels), select)
        mixed = mixed.astype(BF16).reshape(images, width, plan.field_lanes)
        for image in range(images):
            out[block * images + image, :, :channels] = cotangent[image]
            out[block * images + image, :, channels:] = mixed[image]


def group_total(values):
    return jnp.sum(jnp.sum(values, axis=0, keepdims=True), axis=1, keepdims=True)


def prepare_kernel(received, vectors, *outs, plan):
    padded, straight, main_table, spare_table = outs[:4]
    sides = (outs[4:7], outs[7:10])
    plane, position, _ = plan.place()
    width, channels, rows, lanes = plan.width, plan.channels, plan.rows, plan.lanes
    padded[:width, :] = jnp.zeros((width, channels), BF16)
    padded[width + rows :, :] = jnp.zeros((width, channels), BF16)
    field = received[:, :, :channels].reshape(rows, channels)
    padded[width : width + rows, :] = field
    lane = iota((1, lanes), 1)
    spans = [
        (order * LANES, plan.channel(plane, position, order)) for order in range(plan.per_block)
    ]
    straight[...] = dot(field, one_hot(iota((channels, 1), 0), plan.targets(lane, spans))).astype(BF16)
    own = plan.per_block * GSIZE
    fields = received[:, :, channels:].reshape(rows, plan.field_lanes)
    for at, (normed_out, factor_out, inverse_out) in enumerate(sides):
        spans = [(order * LANES, at * own + order * GSIZE) for order in range(plan.per_block)]
        select = one_hot(iota((plan.field_lanes, 1), 0), plan.targets(lane, spans))
        values = dot(fields, select)
        for order in range(plan.per_block):
            part = slice(order * LANES, (order + 1) * LANES)
            first = plan.channel(plane, position, order)
            gain = jnp.zeros((1, GSIZE), F32)
            shift = jnp.zeros((1, GSIZE), F32)
            for group in range(GROUPS):
                span = slice(group * GSIZE, (group + 1) * GSIZE)
                found = first == group * GSIZE
                gain = jnp.where(found, vectors[2 * at : 2 * at + 1, span], gain)
                shift = jnp.where(found, vectors[2 * at + 1 : 2 * at + 2, span], shift)
            rest = jnp.zeros((1, LANES - GSIZE), F32)
            gain = jnp.concatenate([gain, rest], axis=1)
            shift = jnp.concatenate([shift, rest], axis=1)
            block = values[:, part]
            average = group_total(block) / plan.number
            meansq = group_total(block * block) / plan.number
            inverse = lax.rsqrt(meansq - average * average + 1e-05)
            normed = (block - average) * inverse
            linear = normed * gain + shift
            logistic = 1.0 / (1.0 + jnp.exp(-linear))
            normed_out[:, part] = normed
            factor_out[:, part] = logistic * (1.0 + linear * (1.0 - logistic)) * gain
            inverse_out[:, part] = jnp.broadcast_to(inverse, (1, LANES))
    column = iota((1, channels), 1)
    row = iota((LANES, 1), 0)
    for step in range(plan.blocks):
        block = position ^ step
        for at, orders in enumerate(plan.mains):
            spans = [
                (local * GSIZE, plan.channel(plane, block, order))
                for local, order in enumerate(orders)
            ]
            main_table[at, step * LANES : (step + 1) * LANES, :] = one_hot(
                plan.targets(row, spans), column
            )
        if plan.spare is not None:
            for half in range(2):
                spans = [(half * GSIZE, plan.channel(plane, block, plan.spare))]
                spare_table[half, step * LANES : (step + 1) * LANES, :] = one_hot(
                    plan.targets(row, spans), column
                )


def load_weights(pieces, weights, plan):
    _, position, core = plan.place()
    for swap, by_order in enumerate(pieces):
        for order, arrays in enumerate(by_order):
            step = 0
            for array in arrays:
                for inner in range(array.shape[0]):
                    chunk = array.shape[2]
                    source = (position ^ step) * plan.images + (core ^ swap)
                    start = pl.multiple_of(source * chunk, 16)
                    weights[:, pl.ds(start, chunk), order * LANES : (order + 1) * LANES] = array[
                        inner
                    ]
                    step += 1


def convolve(padded, weights, width, part):
    rows = padded.shape[0] - 2 * width
    total = None
    for down in range(3):
        window = padded[(2 - down) * width : (2 - down) * width + rows, :]
        term = dot(window, weights[down, :, part])
        total = term if total is None else total + term
    return total


def fold_sides(total, width):
    rows = total.shape[0]
    column = lax.rem(iota((rows, 1), 0), width)
    first = jnp.where(column == width - 1, 0.0, pltpu.roll(total, rows - 1, 0))
    last = pltpu.roll(pltpu.roll(total, LANES - 2 * GSIZE, 1), 1, 0)
    last = jnp.where(column == 0, 0.0, last)
    return first + pltpu.roll(total, LANES - GSIZE, 1) + last


def norm_backward(incoming, normed, factor, inverse, number):
    scaled = incoming * factor
    first = group_total(scaled) / number
    second = group_total(scaled * normed) / number
    grad = inverse * (scaled - first - normed * second)
    return jnp.where(iota((1, LANES), 1) < GSIZE, grad, 0.0)


def side_by_side(parts):
    total = parts[0]
    for at, part in enumerate(parts[1:]):
        total = total + pltpu.roll(part, (at + 1) * GSIZE, 1)
    return total.astype(BF16)


def block_backward(padded, weights, normed, factor, inverse, plan):
    grads = []
    pair = 2 if plan.per_block % 2 == 0 else 1
    for start in range(0, plan.per_block, pair):
        total = convolve(padded, weights, plan.width, slice(start * LANES, (start + pair) * LANES))
        for at in range(pair):
            part = slice((start + at) * LANES, (start + at + 1) * LANES)
            incoming = fold_sides(total[:, at * LANES : (at + 1) * LANES], plan.width)
            grads.append(
                norm_backward(incoming, normed[:, part], factor[:, part], inverse[:, part], plan.number)
            )
    return grads


def hidden_kernel(padded, normed, factor, inverse, *rest, layout, plan):
    out, weights = rest[layout.total :]
    layout.fill(rest[: layout.total], weights, plan)
    grads = block_backward(padded, weights, normed, factor, inverse, plan)
    rows, half = plan.rows, plan.rows // 2
    for at, orders in enumerate(plan.mains):
        out[at * rows : (at + 1) * rows, :] = side_by_side([grads[order] for order in orders])
    if plan.spare is not None:
        grad = grads[plan.spare]
        out[len(plan.mains) * rows :, :] = side_by_side([grad[:half], grad[half:]])


def unpack(pieces, main_table, spare_table, rows, plan):
    total = None
    for at in range(len(plan.mains)):
        wide = jnp.concatenate([piece[at * rows : (at + 1) * rows, :] for piece in pieces], axis=1)
        term = dot(wide, main_table[at])
        total = term if total is None else total + term
    halves = [None, None] if total is None else [total[: rows // 2], total[rows // 2 :]]
    if plan.spare is not None:
        base = len(plan.mains) * rows
        wide = jnp.concatenate([piece[base : base + rows // 2, :] for piece in pieces], axis=1)
        for half in range(2):
            term = dot(wide, spare_table[half])
            halves[half] = term if halves[half] is None else halves[half] + term
    return [half.astype(BF16) for half in halves]


def latent_kernel(straight, main_table, spare_table, normed, factor, inverse, *rest, layout, plan):
    blocks = plan.blocks
    pieces = rest[:blocks]
    out, weights, padded = rest[blocks + layout.total :]
    layout.fill(rest[blocks : blocks + layout.total], weights, plan)
    width, rows, half = plan.width, plan.rows, plan.rows // 2
    padded[:width, :] = jnp.zeros((width, plan.channels), BF16)
    padded[width + rows :, :] = jnp.zeros((width, plan.channels), BF16)
    low, high = unpack(pieces, main_table, spare_table, rows, plan)
    padded[width : width + half, :] = low
    padded[width + half : width + rows, :] = high
    grads = block_backward(padded, weights, normed, factor, inverse, plan)
    for order in range(plan.per_block):
        grads[order] = straight[:, order * LANES : (order + 1) * LANES].astype(F32) + grads[order]
    for at, orders in enumerate(plan.mains):
        value = side_by_side([grads[order] for order in orders])
        out[:, at * width : (at + 1) * width, :] = value.reshape(plan.height, width, LANES)
    if plan.spare is not None:
        grad = grads[plan.spare].reshape(plan.height, width, LANES)
        parts = [
            grad[:, at * width // 2 : (at + 1) * width // 2, :].reshape(half, LANES) for at in range(2)
        ]
        value = side_by_side(parts).reshape(plan.height, width // 2, LANES)
        out[:, len(plan.mains) * width :, :] = value


def spread_kernel(received, main_table, spare_table, out, *, plan):
    position = plan.place()[1]
    for image in range(plan.images):
        pieces = [
            received[(position ^ step) * plan.images + image] for step in range(plan.blocks)
        ]
        low, high = unpack(pieces, main_table, spare_table, plan.width, plan)
        out[image, : plan.width // 2, :] = low
        out[image, plan.width // 2 :, :] = high


class Layout:
    def __init__(self, pieces):
        self.dynamic = isinstance(pieces, list)
        if self.dynamic:
            self.counts = [[len(arrays) for arrays in by_order] for by_order in pieces]
            self.flat = [array for by_order in pieces for arrays in by_order for array in arrays]
        else:
            self.flat = [pieces]
        self.total = len(self.flat)

    def fill(self, flat, weights, plan):
        if not self.dynamic:
            weights[...] = flat[0][...]
            return
        flat, nested = list(flat), []
        for counts in self.counts:
            nested.append([[flat.pop(0) for _ in range(count)] for count in counts])
        load_weights(nested, weights, plan)


def flip(array, axis, mask):
    return lax.ppermute(array, axis, [(i, i ^ mask) for i in range(lax.axis_size(axis))])


def plane_pieces(filter_two, filter_one, plan):
    out = [((2, 3, filter_two.shape[2], LANES), BF16)] * plan.blocks
    mine = call(functools.partial(pack_filters_kernel, plan=plan), out, [filter_two, filter_one])
    return [mine[0]] + [
        flip(mine[turn], "rows", turn * plan.images) for turn in range(1, plan.blocks)
    ]


def gathered_filter(mine, chunks):
    own = [jnp.stack([mine[turn] for turn in chunk]) for chunk in chunks]
    far = [flip(piece, "dp", 2) for piece in own]
    near = [flip(piece, "dp", 1) for piece in own]
    last = [flip(piece, "dp", 1) for piece in far]
    orders = [own, near, far, last]
    swapped = [[flip(piece, "rows", 1) for piece in order] for order in orders]
    return [orders, swapped]


def assembled_filter(taps, plan):
    count, _, chunk = taps.shape
    blocks, per_block, sources = plan.blocks, plan.per_block, plan.height
    whole = lax.all_gather(taps, "dp", axis=1, tiled=True)
    whole = whole.reshape(count, blocks, per_block * GSIZE, chunk)
    whole = jnp.repeat(jnp.moveaxis(whole, 1, 0), plan.images, axis=0)
    whole = lax.all_to_all(whole, "rows", 0, 0, tiled=True)
    whole = whole.reshape(sources, 3, 3, per_block, GSIZE, chunk)
    whole = jnp.transpose(whole, (1, 0, 5, 3, 2, 4)).reshape(3, sources * chunk, per_block, 3 * GSIZE)
    whole = jnp.pad(whole, ((0, 0), (0, 0), (0, 0), (0, LANES - 3 * GSIZE)))
    return whole.reshape(3, sources * chunk, per_block * LANES)


def step(
    latent, hidden, cotangent, filter_one, filter_two, gain_one, shift_one, gain_two, shift_two
):
    images, _, width, channels = latent.shape
    plan = Plan(images, width, channels)
    rows, lanes = plan.rows, plan.lanes

    if plan.fast:
        mine = plane_pieces(filter_two, filter_one, plan)
        two = Layout(gathered_filter([piece[0] for piece in mine], CHUNKS_TWO))
        one = Layout(gathered_filter([piece[1] for piece in mine], CHUNKS_ONE))
    else:
        two = Layout(assembled_filter(filter_two, plan))
        one = Layout(assembled_filter(filter_one, plan))
    (sent,) = call(
        functools.partial(pack_fields_kernel, plan=plan),
        [((plan.height, width, channels + plan.field_lanes), BF16)],
        [cotangent[:, 0], hidden[:, 0], latent[:, 0]],
    )
    received = lax.all_to_all(sent, "rows", 0, 0, tiled=True)
    vectors = jnp.stack([gain_two, shift_two, gain_one, shift_one])
    table = plan.blocks * LANES
    side = [((rows, lanes), F32), ((rows, lanes), F32), ((1, lanes), F32)]
    prepared = call(
        functools.partial(prepare_kernel, plan=plan),
        [
            ((rows + 2 * width, channels), BF16),
            ((rows, lanes), BF16),
            ((max(len(plan.mains), 1), table, channels), BF16),
            ((2, table, channels), BF16),
        ]
        + side
        + side,
        [received, vectors],
    )
    padded, straight, main_table, spare_table = prepared[:4]
    weights = pltpu.VMEM((3, channels, lanes), BF16)
    inputs = [padded, *prepared[4:7], *two.flat]
    (grad,) = call(
        functools.partial(hidden_kernel, layout=two, plan=plan),
        [((plan.packed_rows(rows), LANES), BF16)],
        inputs,
        held=range(len(inputs)),
        scratch=[weights],
    )
    grads = [grad] + [flip(grad, "rows", turn * images) for turn in range(1, plan.blocks)]
    inputs = [straight, main_table, spare_table, *prepared[7:10], *grads, *one.flat]
    (result,) = call(
        functools.partial(latent_kernel, layout=one, plan=plan),
        [((plan.height, plan.packed_rows(width), LANES), BF16)],
        inputs,
        held=range(len(inputs)),
        scratch=[weights, pltpu.VMEM((rows + 2 * width, channels), BF16)],
    )
    result = lax.all_to_all(result, "rows", 0, 0, tiled=True)
    (out,) = call(
        functools.partial(spread_kernel, plan=plan),
        [((images, width, channels), BF16)],
        [result, main_table, spare_table],
        held=(1, 2),
        space=pl.ANY,
    )
    return out[:, None]


def solution(mesh):
    in_specs = (
        P("dp", "rows", None, None),
        P("dp", "rows", None, None),
        P("dp", "rows", None, None),
        P(None, "dp", "rows"),
        P(None, "dp", "rows"),
        P(),
        P(),
        P(),
        P(),
    )
    out_specs = P("dp", "rows", None, None)
    return jax.shard_map(step, mesh=mesh, in_specs=in_specs, out_specs=out_specs, check_vma=False)
```

```python
import functools

import jax
import jax.numpy as jnp
from jax import lax
from jax.experimental import pallas as pl
from jax.experimental.pallas import tpu as pltpu
from jax.sharding import PartitionSpec as P


GROUPS = 16
GSIZE = 40
LANES = 128


CHUNKS_TWO = ((0, 1), (2, 3))
CHUNKS_ONE = ((0, 1, 2, 3),)

F32 = jnp.float32
BF16 = jnp.bfloat16


def up(number, unit):
    return -(-number // unit) * unit


def one_hot(source, target):
    return jnp.where(source == target, 1.0, 0.0).astype(BF16)


def dot(left, right):
    return jnp.dot(left, right, preferred_element_type=F32)


def iota(shape, axis):
    return lax.broadcasted_iota(jnp.int32, shape, axis)


class Plan:
    def __init__(self, images, width, channels):
        self.images, self.width, self.channels = images, width, channels
        self.height, self.planes = lax.axis_size("rows"), lax.axis_size("dp")
        self.rows = self.height * width
        self.blocks = self.height // images
        self.per_block = GROUPS // self.blocks
        self.number = float(self.rows * GSIZE)
        self.fast = (
            self.planes == 4 and images == 2 and self.blocks == 4 and self.per_block == self.planes
        )
        self.lanes = self.per_block * LANES
        self.field_lanes = up(2 * self.per_block * GSIZE, LANES)
        three = LANES // GSIZE
        self.mains = [
            list(range(start, min(start + three, self.per_block)))
            for start in range(0, self.per_block, three)
        ]
        self.spare = self.mains.pop()[0] if len(self.mains[-1]) == 1 else None

    def packed_rows(self, rows):
        return len(self.mains) * rows + (rows // 2 if self.spare is not None else 0)

    def place(self):
        here = lax.axis_index("rows")
        return lax.axis_index("dp"), here // self.images, here % self.images

    def channel(self, plane, block, order):
        if self.fast:
            return (order ^ plane) * (self.channels // self.planes) + block * GSIZE
        return (block * self.per_block + order) * GSIZE

    def targets(self, index, spans):
        target = jnp.full(index.shape, -1, jnp.int32)
        for start, channel in spans:
            inside = (index >= start) & (index < start + GSIZE)
            target = jnp.where(inside, channel + index - start, target)
        return target


def call(body, out, inputs, held=(), scratch=(), space=pltpu.VMEM):
    kinds = {pltpu.VMEM: pltpu.VMEM, pl.ANY: jax.ShapeDtypeStruct}
    outs = [kinds[space](shape, dtype) for shape, dtype in out]
    inputs = [
        pltpu.with_memory_space_constraint(value, pltpu.VMEM) if at in held else value
        for at, value in enumerate(inputs)
    ]
    vmem = pl.BlockSpec(memory_space=pltpu.VMEM)
    return pl.pallas_call(
        body,
        out_shape=outs,
        in_specs=[vmem] * len(inputs),
        out_specs=[vmem] * len(outs),
        scratch_shapes=list(scratch),
        compiler_params=pltpu.CompilerParams(vmem_limit_bytes=24 * 1024 * 1024),
    )(*inputs)


def pack_kernel(first, second, cotangent, hidden, latent, *rest, plan):
    outs, sent = rest[: plan.blocks], rest[plan.blocks]
    taps_held, fields_held, sent_held, semaphores = rest[plan.blocks + 1 :]
    copies = []
    for at, source in enumerate((cotangent, hidden, latent)):
        copies.append(pltpu.make_async_copy(source, fields_held.at[at], semaphores.at[at]))
    if plan.fast:
        for at, source in enumerate((first, second)):
            copies.append(pltpu.make_async_copy(source, taps_held.at[at], semaphores.at[3 + at]))
    for copy in copies:
        copy.start()
    plane, position, _ = plan.place()
    images, width, channels = plan.images, plan.width, plan.channels
    own = plan.per_block * GSIZE
    rows = iota((channels, 1), 0)
    lane = iota((1, plan.field_lanes), 1)
    selects = []
    for block in range(plan.blocks):
        for at in range(2):
            spans = [
                (at * own + order * GSIZE, plan.channel(plane, block, order))
                for order in range(plan.per_block)
            ]
            selects.append(one_hot(rows, plan.targets(lane, spans)))
    for copy in copies[:3]:
        copy.wait()
    for block in range(plan.blocks):
        mixed = jnp.zeros((images * width, plan.field_lanes), F32)
        for at in range(2):
            field = fields_held[1 + at].reshape(images * width, channels)
            mixed = mixed + dot(field, selects[2 * block + at])
        mixed = mixed.astype(BF16).reshape(images, width, plan.field_lanes)
        for image in range(images):
            sent_held[block * images + image, :, :channels] = fields_held[0, image]
            sent_held[block * images + image, :, channels:] = mixed[image]
    back = pltpu.make_async_copy(sent_held, sent, semaphores.at[5])
    back.start()
    if plan.fast:
        chunk = first.shape[2]
        for at in range(2):
            copies[3 + at].wait()
            parts = []
            for block in range(plan.blocks):
                columns = []
                for down in range(3):
                    pieces = [
                        taps_held[at, 3 * down + side, block * GSIZE : (block + 1) * GSIZE, :].astype(F32)
                        for side in range(3)
                    ]
                    pieces.append(jnp.zeros((LANES - 3 * GSIZE, chunk), F32))
                    columns.append(jnp.concatenate(pieces, axis=0).T.astype(BF16))
                parts.append(columns)
            for turn, out in enumerate(outs):
                wanted = position ^ turn
                for down in range(3):
                    value = parts[0][down]
                    for block in range(1, plan.blocks):
                        value = jnp.where(wanted == block, parts[block][down], value)
                    out[at, down] = value
    else:
        for out in outs:
            out[...] = jnp.zeros(out.shape, BF16)
    back.wait()


def pack(first, second, cotangent, hidden, latent, plan):
    taps = first.shape
    piece = (2, 3, taps[2], LANES) if plan.fast else (8, LANES)
    held = taps if plan.fast else (1, 8, LANES)
    sent = (plan.height, plan.width, plan.channels + plan.field_lanes)
    field = (plan.images, plan.width, plan.channels)
    vmem, anywhere = pl.BlockSpec(memory_space=pltpu.VMEM), pl.BlockSpec(memory_space=pl.ANY)
    inputs = (first, second, cotangent, hidden, latent)
    return pl.pallas_call(
        functools.partial(pack_kernel, plan=plan),
        out_shape=[pltpu.VMEM(piece, BF16)] * plan.blocks + [jax.ShapeDtypeStruct(sent, BF16)],
        in_specs=[anywhere] * 5,
        out_specs=[vmem] * plan.blocks + [anywhere],
        scratch_shapes=[
            pltpu.VMEM((2, *held), BF16),
            pltpu.VMEM((3, *field), BF16),
            pltpu.VMEM(sent, BF16),
            pltpu.SemaphoreType.DMA((6,)),
        ],
        compiler_params=pltpu.CompilerParams(vmem_limit_bytes=24 * 1024 * 1024),
        name="pack",
    )(*(pltpu.with_memory_space_constraint(value, pltpu.HBM) for value in inputs))


def group_total(values):
    return jnp.sum(jnp.sum(values, axis=0, keepdims=True), axis=1, keepdims=True)


def prepare_kernel(received, vectors, *outs, plan):
    padded, straight, main_table, spare_table = outs[:4]
    sides = (outs[4:7], outs[7:10])
    plane, position, _ = plan.place()
    width, channels, rows, lanes = plan.width, plan.channels, plan.rows, plan.lanes
    padded[:width, :] = jnp.zeros((width, channels), BF16)
    padded[width + rows :, :] = jnp.zeros((width, channels), BF16)
    field = received[:, :, :channels].reshape(rows, channels)
    padded[width : width + rows, :] = field
    lane = iota((1, lanes), 1)
    spans = [
        (order * LANES, plan.channel(plane, position, order)) for order in range(plan.per_block)
    ]
    straight[...] = dot(field, one_hot(iota((channels, 1), 0), plan.targets(lane, spans))).astype(BF16)
    own = plan.per_block * GSIZE
    fields = received[:, :, channels:].reshape(rows, plan.field_lanes)
    for at, (normed_out, factor_out, inverse_out) in enumerate(sides):
        spans = [(order * LANES, at * own + order * GSIZE) for order in range(plan.per_block)]
        select = one_hot(iota((plan.field_lanes, 1), 0), plan.targets(lane, spans))
        values = dot(fields, select)
        for order in range(plan.per_block):
            part = slice(order * LANES, (order + 1) * LANES)
            first = plan.channel(plane, position, order)
            gain = jnp.zeros((1, GSIZE), F32)
            shift = jnp.zeros((1, GSIZE), F32)
            for group in range(GROUPS):
                span = slice(group * GSIZE, (group + 1) * GSIZE)
                found = first == group * GSIZE
                gain = jnp.where(found, vectors[2 * at : 2 * at + 1, span], gain)
                shift = jnp.where(found, vectors[2 * at + 1 : 2 * at + 2, span], shift)
            rest = jnp.zeros((1, LANES - GSIZE), F32)
            gain = jnp.concatenate([gain, rest], axis=1)
            shift = jnp.concatenate([shift, rest], axis=1)
            block = values[:, part]
            average = group_total(block) / plan.number
            meansq = group_total(block * block) / plan.number
            inverse = lax.rsqrt(meansq - average * average + 1e-05)
            normed = (block - average) * inverse
            linear = normed * gain + shift
            logistic = 1.0 / (1.0 + jnp.exp(-linear))
            normed_out[:, part] = normed
            factor_out[:, part] = logistic * (1.0 + linear * (1.0 - logistic)) * gain
            inverse_out[:, part] = jnp.broadcast_to(inverse, (1, LANES))
    column = iota((1, channels), 1)
    row = iota((LANES, 1), 0)
    for step in range(plan.blocks):
        block = position ^ step
        for at, orders in enumerate(plan.mains):
            spans = [
                (local * GSIZE, plan.channel(plane, block, order))
                for local, order in enumerate(orders)
            ]
            main_table[at, step * LANES : (step + 1) * LANES, :] = one_hot(
                plan.targets(row, spans), column
            )
        if plan.spare is not None:
            for half in range(2):
                spans = [(half * GSIZE, plan.channel(plane, block, plan.spare))]
                spare_table[half, step * LANES : (step + 1) * LANES, :] = one_hot(
                    plan.targets(row, spans), column
                )


def load_weights(pieces, weights, orders, plan):
    _, position, core = plan.place()
    for swap, by_order in enumerate(pieces):
        for at, order in enumerate(orders):
            turn = 0
            for array in by_order[order]:
                for inner in range(array.shape[0]):
                    chunk = array.shape[2]
                    source = (position ^ turn) * plan.images + (core ^ swap)
                    start = pl.multiple_of(source * chunk, 16)
                    weights[:, pl.ds(start, chunk), at * LANES : (at + 1) * LANES] = array[inner]
                    turn += 1


def convolve(padded, weights, width, part):
    rows = padded.shape[0] - 2 * width
    total = None
    for down in range(3):
        window = padded[(2 - down) * width : (2 - down) * width + rows, :]
        term = dot(window, weights[down, :, part])
        total = term if total is None else total + term
    return total


def fold_sides(total, width):
    rows = total.shape[0]
    column = lax.rem(iota((rows, 1), 0), width)
    first = jnp.where(column == width - 1, 0.0, pltpu.roll(total, rows - 1, 0))
    last = pltpu.roll(pltpu.roll(total, LANES - 2 * GSIZE, 1), 1, 0)
    last = jnp.where(column == 0, 0.0, last)
    return first + pltpu.roll(total, LANES - GSIZE, 1) + last


def norm_backward(incoming, normed, factor, inverse, number):
    scaled = incoming * factor
    first = group_total(scaled) / number
    second = group_total(scaled * normed) / number
    grad = inverse * (scaled - first - normed * second)
    return jnp.where(iota((1, LANES), 1) < GSIZE, grad, 0.0)


def side_by_side(parts):
    total = parts[0]
    for at, part in enumerate(parts[1:]):
        total = total + pltpu.roll(part, (at + 1) * GSIZE, 1)
    return total.astype(BF16)


def block_backward(padded, weights, normed, factor, inverse, orders, plan):
    grads, start = [], 0
    while start < len(orders):
        pair = min(2, len(orders) - start)
        total = convolve(padded, weights, plan.width, slice(start * LANES, (start + pair) * LANES))
        for at in range(pair):
            order = orders[start + at]
            part = slice(order * LANES, (order + 1) * LANES)
            incoming = fold_sides(total[:, at * LANES : (at + 1) * LANES], plan.width)
            grads.append(
                norm_backward(incoming, normed[:, part], factor[:, part], inverse[:, part], plan.number)
            )
        start += pair
    return grads


def hidden_kernel(padded, normed, factor, inverse, *rest, layout, orders, plan):
    count = layout.total(orders)
    out, weights = rest[count:]
    layout.fill(rest[:count], weights, orders, plan)
    grads = block_backward(padded, weights, normed, factor, inverse, orders, plan)
    if len(orders) > 1:
        out[...] = side_by_side(grads)
    else:
        half = plan.rows // 2
        out[...] = side_by_side([grads[0][:half], grads[0][half:]])


def assemble_kernel(*rest, layout, orders, plan):
    layout.fill(rest[:-1], rest[-1], orders, plan)


def unpack(mains, spare, main_table, spare_table, rows):
    halves = [None, None]
    for at, pieces in enumerate(mains):
        term = dot(jnp.concatenate(pieces, axis=1), main_table[at])
        for half in range(2):
            part = term[half * (rows // 2) : (half + 1) * (rows // 2)]
            halves[half] = part if halves[half] is None else halves[half] + part
    if spare:
        wide = jnp.concatenate(spare, axis=1)
        for half in range(2):
            term = dot(wide, spare_table[half])
            halves[half] = term if halves[half] is None else halves[half] + term
    return [half.astype(BF16) for half in halves]


def latent_kernel(straight, main_table, spare_table, weights, normed, factor, inverse, *rest, plan):
    blocks = plan.blocks
    out, padded = rest[-2:]
    width, rows, half = plan.width, plan.rows, plan.rows // 2
    padded[:width, :] = jnp.zeros((width, plan.channels), BF16)
    padded[width + rows :, :] = jnp.zeros((width, plan.channels), BF16)
    pieces = [[piece[...] for piece in rest[at : at + blocks]] for at in range(0, len(rest) - 2, blocks)]
    mains, spare = pieces[: len(plan.mains)], pieces[len(plan.mains) :]
    low, high = unpack(mains, spare[0] if spare else None, main_table, spare_table, rows)
    padded[width : width + half, :] = low
    padded[width + half : width + rows, :] = high
    orders = list(range(plan.per_block))
    grads = block_backward(padded, weights, normed, factor, inverse, orders, plan)
    for order in orders:
        grads[order] = straight[:, order * LANES : (order + 1) * LANES].astype(F32) + grads[order]
    for at, orders in enumerate(plan.mains):
        value = side_by_side([grads[order] for order in orders])
        out[:, at * width : (at + 1) * width, :] = value.reshape(plan.height, width, LANES)
    if plan.spare is not None:
        grad = grads[plan.spare].reshape(plan.height, width, LANES)
        parts = [
            grad[:, at * width // 2 : (at + 1) * width // 2, :].reshape(half, LANES) for at in range(2)
        ]
        value = side_by_side(parts).reshape(plan.height, width // 2, LANES)
        out[:, len(plan.mains) * width :, :] = value


def spread_kernel(received, main_table, spare_table, out, *, plan):
    position = plan.place()[1]
    width, base = plan.width, len(plan.mains) * plan.width
    for image in range(plan.images):
        pieces = [
            received[(position ^ turn) * plan.images + image] for turn in range(plan.blocks)
        ]
        mains = [
            [piece[at * width : (at + 1) * width, :] for piece in pieces]
            for at in range(len(plan.mains))
        ]
        spare = [piece[base:, :] for piece in pieces] if plan.spare is not None else None
        low, high = unpack(mains, spare, main_table, spare_table, width)
        out[image, : width // 2, :] = low
        out[image, width // 2 :, :] = high


class Layout:
    def __init__(self, pieces):
        self.pieces = pieces
        self.dynamic = isinstance(pieces, list)

    def inputs(self, orders):
        if not self.dynamic:
            return [self.pieces]
        return [array for by_order in self.pieces for order in orders for array in by_order[order]]

    def total(self, orders):
        return len(self.inputs(orders))

    def fill(self, flat, weights, orders, plan):
        if not self.dynamic:
            for at, order in enumerate(orders):
                weights[:, :, at * LANES : (at + 1) * LANES] = flat[0][
                    :, :, order * LANES : (order + 1) * LANES
                ]
            return
        flat, nested = list(flat), []
        for by_order in self.pieces:
            nested.append({order: [flat.pop(0) for _ in by_order[order]] for order in orders})
        load_weights(nested, weights, orders, plan)


def flip(array, axis, mask):
    return lax.ppermute(array, axis, [(i, i ^ mask) for i in range(lax.axis_size(axis))])


def gathered_filter(mine, chunks):
    own = [jnp.stack([mine[turn] for turn in chunk]) for chunk in chunks]
    far = [flip(piece, "dp", 2) for piece in own]
    near = [flip(piece, "dp", 1) for piece in own]
    last = [flip(piece, "dp", 1) for piece in far]
    orders = [own, near, far, last]
    swapped = [[flip(piece, "rows", 1) for piece in order] for order in orders]
    return [orders, swapped]


def assembled_filter(taps, plan):
    count, _, chunk = taps.shape
    blocks, per_block, sources = plan.blocks, plan.per_block, plan.height
    whole = lax.all_gather(taps, "dp", axis=1, tiled=True)
    whole = whole.reshape(count, blocks, per_block * GSIZE, chunk)
    whole = jnp.repeat(jnp.moveaxis(whole, 1, 0), plan.images, axis=0)
    whole = lax.all_to_all(whole, "rows", 0, 0, tiled=True)
    whole = whole.reshape(sources, 3, 3, per_block, GSIZE, chunk)
    whole = jnp.transpose(whole, (1, 0, 5, 3, 2, 4)).reshape(3, sources * chunk, per_block, 3 * GSIZE)
    whole = jnp.pad(whole, ((0, 0), (0, 0), (0, 0), (0, LANES - 3 * GSIZE)))
    return whole.reshape(3, sources * chunk, per_block * LANES)


def step(
    latent, hidden, cotangent, filter_one, filter_two, gain_one, shift_one, gain_two, shift_two
):
    images, _, width, channels = latent.shape
    plan = Plan(images, width, channels)
    rows, lanes = plan.rows, plan.lanes

    *packed, sent = pack(filter_two, filter_one, cotangent[:, 0], hidden[:, 0], latent[:, 0], plan)
    if plan.fast:
        mine = [packed[0]] + [
            flip(packed[turn], "rows", turn * images) for turn in range(1, plan.blocks)
        ]
        two = Layout(gathered_filter([piece[0] for piece in mine], CHUNKS_TWO))
        one = Layout(gathered_filter([piece[1] for piece in mine], CHUNKS_ONE))
    else:
        two = Layout(assembled_filter(filter_two, plan))
        one = Layout(assembled_filter(filter_one, plan))
    received = lax.all_to_all(sent, "rows", 0, 0, tiled=True)
    vectors = jnp.stack([gain_two, shift_two, gain_one, shift_one])
    table = plan.blocks * LANES
    side = [((rows, lanes), F32), ((rows, lanes), F32), ((1, lanes), F32)]
    prepared = call(
        functools.partial(prepare_kernel, plan=plan),
        [
            ((rows + 2 * width, channels), BF16),
            ((rows, lanes), BF16),
            ((max(len(plan.mains), 1), table, channels), BF16),
            ((2, table, channels), BF16),
        ]
        + side
        + side,
        [received, vectors],
    )
    padded, straight, main_table, spare_table = prepared[:4]
    parts = plan.mains + ([[plan.spare]] if plan.spare is not None else [])
    grads = []
    for orders in parts:
        inputs = [padded, *prepared[4:7], *two.inputs(orders)]
        (grad,) = call(
            functools.partial(hidden_kernel, layout=two, orders=orders, plan=plan),
            [((rows if len(orders) > 1 else rows // 2, LANES), BF16)],
            inputs,
            held=range(len(inputs)),
            scratch=[pltpu.VMEM((3, channels, len(orders) * LANES), BF16)],
        )
        grads.append(grad)
        grads += [flip(grad, "rows", turn * images) for turn in range(1, plan.blocks)]
    orders = list(range(plan.per_block))
    inputs = one.inputs(orders)
    (weights,) = call(
        functools.partial(assemble_kernel, layout=one, orders=orders, plan=plan),
        [((3, channels, lanes), BF16)],
        inputs,
        held=range(len(inputs)),
    )
    inputs = [straight, main_table, spare_table, weights, *prepared[7:10], *grads]
    (result,) = call(
        functools.partial(latent_kernel, plan=plan),
        [((plan.height, plan.packed_rows(width), LANES), BF16)],
        inputs,
        held=range(len(inputs)),
        scratch=[pltpu.VMEM((rows + 2 * width, channels), BF16)],
    )
    result = lax.all_to_all(result, "rows", 0, 0, tiled=True)
    (out,) = call(
        functools.partial(spread_kernel, plan=plan),
        [((images, width, channels), BF16)],
        [result, main_table, spare_table],
        held=(1, 2),
        space=pl.ANY,
    )
    return out[:, None]


def solution(mesh):
    in_specs = (
        P("dp", "rows", None, None),
        P("dp", "rows", None, None),
        P("dp", "rows", None, None),
        P(None, "dp", "rows"),
        P(None, "dp", "rows"),
        P(),
        P(),
        P(),
        P(),
    )
    out_specs = P("dp", "rows", None, None)
    return jax.shard_map(step, mesh=mesh, in_specs=in_specs, out_specs=out_specs, check_vma=False)
```
